128 devices in a mesh: ic: 4 (over z_lo, core), member: 2 (over z_hi), lat: 16 (over x, y).
Axes of the slice: x: 4, y: 4, z: 4 (z_hi: 2, z_lo: 2; z = z_hi * 2 + z_lo), core: 2. Of those that a mesh axis runs over, the one named last changes fastest.
Arguments:
- state: bfloat16 [8, 640, 32, 2560], P(('ic', 'member'), 'lat'), parts along dimension 0, may hold values from -6 to 6
- target: bfloat16 [2560, 32, 2560], P(('ic', 'lat')), parts along dimension 0, may hold values from -6 to 6
- noise: float32 [8, 640, 32, 320], P(('ic', 'member'), 'lat'), parts along dimension 0, may hold values from -4 to 4
- gain: float32 [640, 320], P('lat'), may hold values from 0.2 to 1
- vertical_mix: float32 [32, 32], replicated, may hold values from -1 to 1
Outputs:
- new_state: bfloat16 [8, 640, 32, 2560], P(('ic', 'member'), 'lat'), parts along dimension 0
- crps: float32 [8, 640, 2560], P(('ic', 'member'), 'lat'), parts along dimension 0
The draws below stay inside these ranges and needn't reach their ends.
There are 4 independent parts, one for each index of `ic`. The reference program is written for one: setup_inputs(seed, part) draws one part's arguments, and reference() takes and returns one part's arrays. A program takes and returns all parts, laid end to end along the dimension named above; an argument that names none is the same for every part. Nothing has to cross between parts.
All inputs are finite; a program needn't handle non-finite values.
Results may differ from the reference program's by a relative error of at most 0.0042.
Values may be sent and summed in bfloat16 or wider, within the bound.
No kernel may reach another device: no remote copies, remote signals or barrier semaphores. Data moves between devices by JAX's collectives and lax.ppermute only.
A program may use at most 128 MiB of HBM per device.

```python
import math
import jax
import jax.numpy as jnp
from jax import lax

NLON = 2560
NLAT = 640
MW = 320
LEVELS = 32
MEMBERS = 2
NK = 320


def shard_levels(key, shape, pieces, low, top_value):
    level = 1.0
    for dim, parts in pieces:
        draws = jax.random.uniform(jax.random.fold_in(jax.random.fold_in(key, 6), dim), (parts,), jnp.float32, low / len(pieces), top_value / len(pieces))
        level = level * jnp.repeat(jnp.exp(draws), shape[dim] // parts).reshape((-1,) + (1,) * (len(shape) - 1 - dim))
    return level


def centred(key, dims, width, bound, shards=(), held_as=jnp.bfloat16):
    result = width * jax.random.normal(key, dims, jnp.float32)
    if shards:
        result = result * shard_levels(key, dims, shards, -0.22, 0.18)
    return jnp.clip(result, -bound, bound).astype(held_as)


def setup_inputs(seed: int = 0, part: int = 0) -> dict:
    seeds = jax.random.split(jax.random.key(seed), 6)
    part_keys = jax.random.split(jax.random.fold_in(seeds[5], part), 6)
    return {
        "state": centred(part_keys[0], (MEMBERS, NLAT, LEVELS, NLON), 1.0, 6.0, ((0, 2), (1, 16))),
        "target": centred(part_keys[1], (NLAT, LEVELS, NLON), 1.0, 6.0, ((0, 16),)),
        "noise": centred(part_keys[2], (MEMBERS, 2 * MW, LEVELS, NK), 0.5, 4.0, ((0, 2), (1, 16)), jnp.float32),
        "gain": jnp.clip(jnp.exp(math.log(1.0) - 1.609438 * jax.random.uniform(seeds[3], (2 * MW, NK), jnp.float32) ** shard_levels(seeds[3], (2 * MW, NK), ((0, 16),), -0.2, 0.2)), 0.2, 1.0),
        "vertical_mix": centred(seeds[4], (LEVELS, LEVELS), LEVELS ** -0.5, 1.0, (), jnp.float32),
    }


def column_info():
    column = jnp.arange(2 * MW, dtype=jnp.int32)
    part = column // MW
    rest = column % MW
    half = MW // 2
    wave = jnp.where(rest < half, 2 * rest + 2 * part, 2 * (rest - half) + 1)
    return (part, wave, rest >= half)

def lon_table():
    part, wave, odd = column_info()
    place = jnp.arange(NLON, dtype=jnp.int32)
    phase = place[:, None] * wave[None, :] % NLON
    angle = phase.astype(jnp.float32) * jnp.float32(2.0 * math.pi / NLON)
    return jnp.where(part[None, :] == 0, jnp.cos(angle), jnp.sin(angle)).astype(jnp.bfloat16)

def lat_bases():
    theta = (jnp.arange(NLAT, dtype=jnp.float32) + 0.5) * jnp.float32(math.pi / NLAT)
    modes = jnp.arange(NLAT // 2, dtype=jnp.float32)
    even = jnp.cos(modes[:, None] * theta[None, :])
    odd = jnp.sin((modes[:, None] + 1.0) * theta[None, :])
    return (even, odd)

def member_score(own, other, truth):
    own = own.astype(jnp.float32)
    other = other.astype(jnp.float32)
    truth = truth.astype(jnp.float32)
    skill = lax.optimization_barrier(jnp.mean(jnp.abs(own - truth), axis=1))
    spread = lax.optimization_barrier(jnp.mean(jnp.abs(own - other), axis=1))
    return skill - 0.5 * spread

def reference(state, target, noise, gain, vertical_mix):
    table = lon_table()
    even, odd_basis = lat_bases()
    part, wave, odd = column_info()
    modes = NLAT // 2
    levels = state.shape[2]
    highest = lax.Precision.HIGHEST
    outputs = []
    for member in range(MEMBERS):
        field = state[member]
        zonal = jnp.dot(field.reshape(NLAT * levels, NLON), table, preferred_element_type=jnp.float32)
        zonal = (zonal * jnp.float32(1.0 / math.sqrt(NLON))).reshape(NLAT, levels * 2 * MW)
        spec_even = jnp.dot(even, zonal, precision=highest).reshape(modes, levels, 2 * MW)
        spec_odd = jnp.dot(odd_basis, zonal, precision=highest).reshape(modes, levels, 2 * MW)
        spectral = jnp.where(odd[None, None, :], spec_odd, spec_even) * jnp.float32(math.sqrt(2.0 / NLAT))
        forced = gain.T[:, None, :] * spectral + jnp.transpose(noise[member], (2, 1, 0))
        flat = forced.reshape(modes, levels * 2 * MW)
        back_even = jnp.dot(even.T, flat, precision=highest).reshape(NLAT, levels, 2 * MW)
        back_odd = jnp.dot(odd_basis.T, flat, precision=highest).reshape(NLAT, levels, 2 * MW)
        back = jnp.where(odd[None, None, :], back_odd, back_even) * jnp.float32(math.sqrt(2.0 / modes))
        back = back.astype(jnp.bfloat16)
        tendency = lax.dot_general(back.reshape(NLAT * levels, 2 * MW), table, (((1,), (1,)), ((), ())), preferred_element_type=jnp.float32)
        tendency = (tendency * jnp.float32(1.0 / math.sqrt(MW))).reshape(NLAT, levels, NLON)
        mixed = jnp.einsum('ab,jbi->jai', vertical_mix, tendency, precision=highest)
        outputs.append((field.astype(jnp.float32) + mixed).astype(jnp.bfloat16))
    new_state = jnp.stack(outputs, axis=0)
    crps = jnp.stack([member_score(new_state[0], new_state[1], target), member_score(new_state[1], new_state[0], target)], axis=0)
    return (new_state, crps)
```

```python
import functools
import math

import jax
import jax.numpy as jnp
import ml_dtypes
import numpy as np
from jax import lax
from jax.experimental import pallas as pl
from jax.experimental.pallas import tpu as pltpu
from jax.sharding import PartitionSpec as P

NLON = 2560
NLAT = 640
MW = 320
LEVELS = 32
NK = 320
NCOL = 2 * MW
LAT = 16
ROWS = NLAT // LAT
OWN = NCOL // LAT
HALF = LEVELS // 2
TILES = OWN // 8
GROUPS = ROWS // 8
BF16 = jnp.bfloat16
F32 = jnp.float32
HIGHEST = lax.Precision.HIGHEST


def column_order():
    n = np.arange(NCOL)
    return 40 * ((n % 128) // 8) + 8 * (n // 128) + n % 8


def lon_table():
    column = column_order()
    part = column // MW
    rest = column % MW
    half = MW // 2
    wave = np.where(rest < half, 2 * rest + 2 * part, 2 * (rest - half) + 1)
    phase = np.arange(NLON)[:, None] * wave[None, :] % NLON
    angle = 2.0 * math.pi / NLON * phase
    table = np.where(part[None, :] == 0, np.cos(angle), np.sin(angle))
    return table.astype(np.float32).astype(ml_dtypes.bfloat16)


def lat_bases():
    theta = (np.arange(NLAT) + 0.5) * (math.pi / NLAT)
    modes = np.arange(NK)
    even = np.cos(modes[:, None] * theta[None, :])
    odd = np.sin((modes[:, None] + 1.0) * theta[None, :])
    both = np.stack([even, odd]).astype(np.float32)
    high = both.astype(ml_dtypes.bfloat16)
    low = (both - high.astype(np.float32)).astype(ml_dtypes.bfloat16)
    return high, low


def swap_groups(v):
    v = list(v)
    lane = lax.broadcasted_iota(jnp.int32, v[0].shape, 1)
    for bit in range(4):
        shift = 8 << bit
        upper = (lane & shift) != 0
        for a in range(16):
            if a & (1 << bit):
                continue
            first, second = v[a], v[a | (1 << bit)]
            v[a] = jnp.where(upper, pltpu.roll(second, shift, 1), first)
            v[a | (1 << bit)] = jnp.where(upper, second, pltpu.roll(first, 128 - shift, 1))
    return v


def forward_kernel(x_ref, table_ref, out_ref, held):
    zonal = jnp.dot(x_ref[...], table_ref[...], preferred_element_type=F32)
    for t in range(TILES):
        for j in range(8):
            held[t, 40 * j : 40 * j + 32, :] = zonal[32 * j : 32 * j + 32, 128 * t : 128 * (t + 1)]
    for t in range(TILES):
        for h in range(2):
            v = [held[t, pl.ds(HALF * h + a, 8, stride=40), :] for a in range(16)]
            lanes = slice(128 * (2 * t + h), 128 * (2 * t + h + 1))
            for q, w in enumerate(swap_groups(v)):
                out_ref[q, :, lanes] = w.astype(BF16)


def forward(field, table):
    rows = field.shape[0]
    return pl.pallas_call(
        forward_kernel,
        grid=(GROUPS,),
        in_specs=[
            pl.BlockSpec((rows // GROUPS, NLON), lambda i: (i, 0)),
            pl.BlockSpec((NLON, NCOL), lambda i: (0, 0)),
        ],
        out_specs=pl.BlockSpec((LAT, 8, OWN * LEVELS), lambda i: (0, i, 0)),
        out_shape=jax.ShapeDtypeStruct((LAT, ROWS, OWN * LEVELS), BF16),
        scratch_shapes=[pltpu.VMEM((TILES, 8 * 40, 128), F32)],
        cost_estimate=pl.CostEstimate(
            flops=2 * rows * NLON * NCOL, bytes_accessed=12_000_000, transcendentals=0
        ),
        name="forward_lon",
    )(field, table)


def prepare_kernel(noise_ref, mix_ref, gain_ref, pick_ref, mixed_ref, wide_ref):
    contract = (((0,), (0,)), ((), ()))
    mixed_ref[...] = lax.dot_general(
        noise_ref[...], mix_ref[...], contract, precision=HIGHEST, preferred_element_type=F32
    )
    wide_ref[...] = lax.dot_general(
        gain_ref[...], pick_ref[...], contract, precision=HIGHEST, preferred_element_type=F32
    )


def prepare(noise, mix, gain, pick):
    wide = OWN * LEVELS
    return pl.pallas_call(
        prepare_kernel,
        grid=(TILES,),
        in_specs=[
            pl.BlockSpec((256, NK), lambda t: (t, 0)),
            pl.BlockSpec((256, 256), lambda t: (0, 0)),
            pl.BlockSpec((OWN, NK), lambda t: (0, 0)),
            pl.BlockSpec((OWN, 256), lambda t: (0, t)),
        ],
        out_specs=[
            pl.BlockSpec((NK, 256), lambda t: (0, t)),
            pl.BlockSpec((NK, 256), lambda t: (0, t)),
        ],
        out_shape=[jax.ShapeDtypeStruct((NK, wide), F32)] * 2,
        cost_estimate=pl.CostEstimate(
            flops=12 * 256 * NK * wide, bytes_accessed=6_000_000, transcendentals=0
        ),
        name="prepare_noise",
    )(noise, mix, gain, pick)


def halves(x):
    high = x.astype(BF16)
    return high, (x - high.astype(F32)).astype(BF16)


def mm(a, b):
    return jnp.dot(a, b, preferred_element_type=F32)


def spectral_kernel(odd, g_ref, bh_ref, bl_ref, th_ref, tl_ref, mh_ref, ml_ref, noise_ref, gain_ref, send_ref, keep_ref):
    g = g_ref[...]
    forced = (mm(bh_ref[0], g) + mm(bl_ref[0], g)) * gain_ref[...]
    high, low = halves(forced)
    mixed = mm(high, mh_ref[...]) + mm(low, mh_ref[...]) + mm(high, ml_ref[...]) + noise_ref[...]
    high, low = halves(mixed)
    back = mm(th_ref[0], high) + mm(th_ref[0], low) + mm(tl_ref[0], high)
    back = (back * F32(math.sqrt(2.0) / NK)).astype(BF16)
    send_ref[...] = back[:, :128]
    keep_ref[...] = back[:, 128:]


def spectral(odd, gathered, bases, mixes, noise, gain):
    def whole(shape):
        return pl.BlockSpec((1,) + shape, lambda t, odd: (odd[0], 0, 0))

    mix_spec = pl.BlockSpec((256, 256), lambda t, odd: (0, 0))
    tile_spec = pl.BlockSpec((NK, 256), lambda t, odd: (0, t))
    half_spec = pl.BlockSpec((NLAT, 128), lambda t, odd: (0, t))
    return pl.pallas_call(
        spectral_kernel,
        grid_spec=pltpu.PrefetchScalarGridSpec(
            num_scalar_prefetch=1,
            grid=(TILES,),
            in_specs=[
                pl.BlockSpec((NLAT, 256), lambda t, odd: (0, t)),
                whole((NK, NLAT)),
                whole((NK, NLAT)),
                whole((NLAT, NK)),
                whole((NLAT, NK)),
                mix_spec,
                mix_spec,
                tile_spec,
                tile_spec,
            ],
            out_specs=[half_spec, half_spec],
        ),
        out_shape=[jax.ShapeDtypeStruct((NLAT, TILES * 128), BF16)] * 2,
        cost_estimate=pl.CostEstimate(
            flops=4_000_000_000, bytes_accessed=10_000_000, transcendentals=0
        ),
        name="spectral_step",
    )(odd, gathered, *bases, *mixes, noise, gain)


def rows_of(coef_ref, held):
    for t in range(TILES):
        v = [coef_ref[q, :, 128 * t : 128 * (t + 1)].astype(F32) for q in range(LAT)]
        for a, w in enumerate(swap_groups(v)):
            held[t, pl.ds(a, 8, stride=24), :] = w
    tiles = [
        jnp.concatenate([held[t, 24 * j : 24 * j + 16, :] for j in range(8)], axis=0)
        for t in range(TILES)
    ]
    return jnp.concatenate(tiles, axis=1).astype(BF16)


CHUNK = 640


def own_kernel(where, coef_ref, state_ref, target_ref, table_ref, *rest):
    new_ref, skill_ref, held = rest[-3:]
    rows = rows_of(coef_ref, held)
    for n in range(0, NLON, CHUNK):
        cut = slice(n, n + CHUNK)
        tendency = mm(rows, table_ref[:, cut]).reshape(8, HALF, CHUNK)
        new = (state_ref[:, :, cut].astype(F32) + tendency).astype(BF16)
        new_ref[:, :, cut] = new
        skill_ref[:, cut] = jnp.sum(
            jnp.abs(new.astype(F32) - target_ref[:, :, cut].astype(F32)), axis=1
        )


def own_step(where, coef, state, target, table, into=None):
    level_spec = pl.BlockSpec((8, HALF, NLON), lambda i, where: (i, where[0], 0))
    extra = [] if into is None else [into]
    return pl.pallas_call(
        own_kernel,
        grid_spec=pltpu.PrefetchScalarGridSpec(
            num_scalar_prefetch=1,
            grid=(GROUPS,),
            in_specs=[
                pl.BlockSpec((LAT, 8, TILES * 128), lambda i, where: (0, i, 0)),
                level_spec,
                level_spec,
                pl.BlockSpec((NCOL, NLON), lambda i, where: (0, 0)),
            ]
            + [pl.BlockSpec(memory_space=pl.ANY) for _ in extra],
            out_specs=[level_spec, pl.BlockSpec((8, NLON), lambda i, where: (i, 0))],
            scratch_shapes=[pltpu.VMEM((TILES, 8 * 24, 128), F32)],
        ),
        out_shape=[
            jax.ShapeDtypeStruct((ROWS, LEVELS, NLON), BF16),
            jax.ShapeDtypeStruct((ROWS, NLON), F32),
        ],
        input_output_aliases={} if into is None else {5: 0},
        cost_estimate=pl.CostEstimate(
            flops=2 * ROWS * HALF * NCOL * NLON, bytes_accessed=14_000_000, transcendentals=0
        ),
        name="own_step",
    )(where, coef, state, target, table, *extra)


def other_kernel(where, coef_ref, state_ref, own_ref, table_ref, spread_ref, held):
    rows = rows_of(coef_ref, held)
    for n in range(0, NLON, CHUNK):
        cut = slice(n, n + CHUNK)
        tendency = mm(rows, table_ref[:, cut]).reshape(8, HALF, CHUNK)
        new = (state_ref[:, :, cut].astype(F32) + tendency).astype(BF16)
        spread_ref[:, cut] = jnp.sum(
            jnp.abs(new.astype(F32) - own_ref[:, :, cut].astype(F32)), axis=1
        )


def other_step(where, coef, state, own, table):
    return pl.pallas_call(
        other_kernel,
        grid_spec=pltpu.PrefetchScalarGridSpec(
            num_scalar_prefetch=1,
            grid=(GROUPS,),
            in_specs=[
                pl.BlockSpec((LAT, 8, TILES * 128), lambda i, where: (0, i, 0)),
                pl.BlockSpec((8, HALF, NLON), lambda i, where: (i, 0, 0)),
                pl.BlockSpec((8, HALF, NLON), lambda i, where: (i, where[0], 0)),
                pl.BlockSpec((NCOL, NLON), lambda i, where: (0, 0)),
            ],
            out_specs=pl.BlockSpec((8, NLON), lambda i, where: (i, 0)),
            scratch_shapes=[pltpu.VMEM((TILES, 8 * 24, 128), F32)],
        ),
        out_shape=jax.ShapeDtypeStruct((ROWS, NLON), F32),
        cost_estimate=pl.CostEstimate(
            flops=2 * ROWS * HALF * NCOL * NLON, bytes_accessed=12_000_000, transcendentals=0
        ),
        name="other_step",
    )(where, coef, state, own, table)


def to_partner(x):
    return lax.ppermute(x, "member", [(0, 1), (1, 0)])


def over_lat(x):
    return lax.all_to_all(x, "lat", split_axis=0, concat_axis=0, tiled=True)


def body(state, target, noise, gain, vertical_mix):
    member = lax.axis_index("member")
    lat = lax.axis_index("lat")
    field = state[0]

    partner_state = to_partner(lax.dynamic_slice_in_dim(field, HALF * (1 - member), HALF, 1))

    table = lon_table()
    sent = forward(field.reshape(ROWS * LEVELS, NLON), jnp.asarray(table))
    gathered = over_lat(sent).reshape(NLAT, OWN * LEVELS)

    mix = jnp.where(member == 1, vertical_mix, jnp.roll(vertical_mix, HALF, axis=0))
    eye = jnp.eye(8, dtype=F32)
    spread = mix.T[:, None, :, None] * eye[None, :, None, :]
    for_noise = jnp.transpose(spread, (1, 0, 2, 3)).reshape(256, 256)
    spread = spread.reshape(256, 256)
    mix_high = spread.astype(BF16)
    mix_low = (spread - lax.reduce_precision(spread, 8, 7)).astype(BF16)
    pick = np.zeros((OWN, OWN * LEVELS), np.float32)
    n = np.arange(OWN * LEVELS)
    pick[8 * (n // 256) + n % 8, n] = math.sqrt(2.0 / NLAT) / math.sqrt(NLON)
    mixed_noise, wide_gain = prepare(
        noise[0].reshape(OWN * LEVELS, NK), for_noise, gain, jnp.asarray(pick)
    )

    high, low = lat_bases()
    bases = [high, low, high.transpose(0, 2, 1), low.transpose(0, 2, 1)]
    odd = (lat % 8 >= 4).astype(jnp.int32).reshape(1)
    give, keep = spectral(
        odd, gathered, [jnp.asarray(b) for b in bases], (mix_high, mix_low), mixed_noise, wide_gain
    )
    give = over_lat(give.reshape(LAT, ROWS, TILES * 128))
    partner_coef = to_partner(give)
    keep = over_lat(keep.reshape(LAT, ROWS, TILES * 128))

    back_table = jnp.asarray(np.ascontiguousarray(table.T))
    mine = member.astype(jnp.int32).reshape(1)
    new, skill_a = own_step(1 - mine, give, field, target, back_table)
    new, skill_b = own_step(mine, keep, field, target, back_table, new)
    part = other_step(mine, partner_coef, partner_state, new, back_table)
    rest = to_partner(part)
    crps = (skill_a + skill_b) * F32(1.0 / LEVELS) - (part + rest) * F32(0.5 / LEVELS)
    return new[None], crps[None]


def solution(mesh):
    placed = (
        P(("ic", "member"), "lat", None, None),
        P(("ic", "lat"), None, None),
        P(("ic", "member"), "lat", None, None),
        P("lat", None),
        P(),
    )
    return jax.shard_map(
        body,
        mesh=mesh,
        in_specs=placed,
        out_specs=(P(("ic", "member"), "lat", None, None), P(("ic", "member"), "lat", None)),
        check_vma=False,
    )
```

```python
import math

import jax
import jax.numpy as jnp
import ml_dtypes
import numpy as np
from jax import lax
from jax.experimental import pallas as pl
from jax.experimental.pallas import tpu as pltpu
from jax.sharding import PartitionSpec as P


NLON = 2560
NLAT = 640
MW = 320
LEVELS = 32
NK = 320
NCOL = 2 * MW
LAT = 16
ROWS = NLAT // LAT
OWN = NCOL // LAT
HALF = LEVELS // 2
TILES = OWN // 8
GROUPS = ROWS // 8
BF16 = jnp.bfloat16
F32 = jnp.float32
HIGHEST = lax.Precision.HIGHEST
OWN_LIMIT = 58 << 20
SMALL_LIMIT = 16 << 20
HBM = pl.BlockSpec(memory_space=pltpu.HBM)
VMEM = pl.BlockSpec(memory_space=pltpu.VMEM)
SMEM = pl.BlockSpec(memory_space=pltpu.SMEM)
FIELD = (ROWS, HALF, NLON)


def column_order():
    n = np.arange(NCOL)
    return 40 * ((n % 128) // 8) + 8 * (n // 128) + n % 8


def lon_table():
    column = column_order()
    part = column // MW
    rest = column % MW
    half = MW // 2
    wave = np.where(rest < half, 2 * rest + 2 * part, 2 * (rest - half) + 1)
    phase = np.arange(NLON)[:, None] * wave[None, :] % NLON
    angle = 2.0 * math.pi / NLON * phase
    table = np.where(part[None, :] == 0, np.cos(angle), np.sin(angle))
    return table.astype(np.float32).astype(ml_dtypes.bfloat16)


def lat_bases():
    theta = (np.arange(NLAT) + 0.5) * (math.pi / NLAT)
    modes = np.arange(NK)
    even = np.cos(modes[:, None] * theta[None, :])
    odd = np.sin((modes[:, None] + 1.0) * theta[None, :])
    both = np.stack([even, odd]).astype(np.float32)
    high = both.astype(ml_dtypes.bfloat16)
    low = (both - high.astype(np.float32)).astype(ml_dtypes.bfloat16)
    return high, low


def turn(x, groups):
    return pltpu.roll(x, 8 * groups % 128, 1) if groups % 16 else x


def swap_groups(v):
    group = lax.broadcasted_iota(jnp.int32, v[0].shape, 1) // 8
    x = [turn(v[-b % 16], -b % 16) for b in range(16)]
    for bit in range(4):
        moved = (group & (1 << bit)) != 0
        x = [jnp.where(moved, x[(g - (1 << bit)) % 16], x[g]) for g in range(16)]
    return [turn(x[g], 16 - g) for g in range(16)]


def forward_kernel(x_ref, table_ref, out_ref, held):
    step = pl.program_id(0)
    now, before = lax.rem(step, 2), lax.rem(step + 1, 2)
    zonal = jnp.dot(x_ref[...], table_ref[...], preferred_element_type=F32)
    for t in range(TILES):
        for h in range(2):
            v = [held[before, t, pl.ds(HALF * h + a, 8, stride=40), :] for a in range(16)]
            lanes = slice(128 * (2 * t + h), 128 * (2 * t + h + 1))
            for q, w in enumerate(swap_groups(v)):
                out_ref[q, :, lanes] = w.astype(BF16)
    for t in range(TILES):
        for j in range(8):
            held[now, t, 40 * j : 40 * j + 32, :] = zonal[
                32 * j : 32 * j + 32, 128 * t : 128 * (t + 1)
            ]


def forward(field, table):
    rows = field.shape[0]
    return pl.pallas_call(
        forward_kernel,
        grid=(GROUPS + 1,),
        in_specs=[
            pl.BlockSpec((rows // GROUPS, NLON), lambda i: (jnp.minimum(i, GROUPS - 1), 0)),
            pl.BlockSpec((NLON, NCOL), lambda i: (0, 0)),
        ],
        out_specs=pl.BlockSpec((LAT, 8, OWN * LEVELS), lambda i: (0, jnp.maximum(i - 1, 0), 0)),
        out_shape=jax.ShapeDtypeStruct((LAT, ROWS, OWN * LEVELS), BF16),
        scratch_shapes=[pltpu.VMEM((2, TILES, 8 * 40, 128), F32)],
        cost_estimate=pl.CostEstimate(
            flops=2 * rows * NLON * NCOL, bytes_accessed=12_000_000, transcendentals=0
        ),
        compiler_params=pltpu.CompilerParams(vmem_limit_bytes=SMALL_LIMIT),
        name="forward_lon",
    )(field, table)


def prepare_kernel(noise_ref, mix_ref, gain_ref, pick_ref, mixed_ref, wide_ref):
    contract = (((0,), (0,)), ((), ()))
    mixed_ref[...] = lax.dot_general(
        noise_ref[...], mix_ref[...], contract, precision=HIGHEST, preferred_element_type=F32
    )
    wide_ref[...] = lax.dot_general(
        gain_ref[...], pick_ref[...], contract, precision=HIGHEST, preferred_element_type=F32
    )


def prepare(noise, mix, gain, pick):
    wide = OWN * LEVELS
    return pl.pallas_call(
        prepare_kernel,
        grid=(TILES,),
        in_specs=[
            pl.BlockSpec((256, NK), lambda t: (t, 0)),
            pl.BlockSpec((256, 256), lambda t: (0, 0)),
            pl.BlockSpec((OWN, NK), lambda t: (0, 0)),
            pl.BlockSpec((OWN, 256), lambda t: (0, t)),
        ],
        out_specs=[
            pl.BlockSpec((NK, 256), lambda t: (0, t)),
            pl.BlockSpec((NK, 256), lambda t: (0, t)),
        ],
        out_shape=[jax.ShapeDtypeStruct((NK, wide), F32)] * 2,
        cost_estimate=pl.CostEstimate(
            flops=12 * 256 * NK * wide, bytes_accessed=6_000_000, transcendentals=0
        ),
        compiler_params=pltpu.CompilerParams(vmem_limit_bytes=SMALL_LIMIT),
        name="prepare_noise",
    )(noise, mix, gain, pick)


def halves(x):
    high = x.astype(BF16)
    return high, (x - high.astype(F32)).astype(BF16)


def mm(a, b):
    return jnp.dot(a, b, preferred_element_type=F32)


def spectral_kernel(odd, g_ref, b_ref, t_ref, mh_ref, ml_ref, noise_ref, gain_ref, send_ref, keep_ref, b, t, noise, gain, sems):
    loads = [
        pltpu.make_async_copy(b_ref.at[odd[0]], b, sems.at[0]),
        pltpu.make_async_copy(gain_ref, gain, sems.at[1]),
        pltpu.make_async_copy(noise_ref, noise, sems.at[2]),
        pltpu.make_async_copy(t_ref.at[odd[0]], t, sems.at[3]),
    ]
    for copy in loads:
        copy.start()
    loads[0].wait()
    for k in range(TILES):
        lanes = slice(256 * k, 256 * (k + 1))
        both = mm(b[...], g_ref[:, lanes])
        if k == 0:
            loads[1].wait()
        forced = (both[:NK] + both[NK:]) * gain[:, lanes]
        high, low = halves(forced)
        both = mm(jnp.concatenate([high, low], axis=0), mh_ref[...])
        if k == 0:
            loads[2].wait()
        mixed = both[:NK] + both[NK:] + mm(high, ml_ref[...]) + noise[:, lanes]
        high, low = halves(mixed)
        if k == 0:
            loads[3].wait()
        both = mm(t[...], high)
        back = both[:NLAT] + both[NLAT:] + mm(t[:NLAT], low)
        back = (back * F32(math.sqrt(2.0) / NK)).astype(BF16)
        send_ref[:, 128 * k : 128 * (k + 1)] = back[:, :128]
        keep_ref[:, 128 * k : 128 * (k + 1)] = back[:, 128:]


def spectral(odd, gathered, bases, mixes, noise, gain):
    return pl.pallas_call(
        spectral_kernel,
        in_specs=[SMEM, VMEM, HBM, HBM, VMEM, VMEM, HBM, HBM],
        out_specs=[VMEM, VMEM],
        out_shape=[jax.ShapeDtypeStruct((NLAT, TILES * 128), BF16)] * 2,
        scratch_shapes=[
            pltpu.VMEM((2 * NK, NLAT), BF16),
            pltpu.VMEM((2 * NLAT, NK), BF16),
            pltpu.VMEM((NK, OWN * LEVELS), F32),
            pltpu.VMEM((NK, OWN * LEVELS), F32),
            pltpu.SemaphoreType.DMA((4,)),
        ],
        cost_estimate=pl.CostEstimate(
            flops=4_000_000_000, bytes_accessed=10_000_000, transcendentals=0
        ),
        compiler_params=pltpu.CompilerParams(vmem_limit_bytes=OWN_LIMIT),
        name="spectral_step",
    )(odd, gathered, *bases, *mixes, noise, gain)


def set_rows(coef_ref, held, rows_ref, groups):
    for i in groups:
        for t in range(TILES):
            lanes = slice(128 * t, 128 * (t + 1))
            v = [coef_ref[q, 8 * i : 8 * i + 8, lanes].astype(F32) for q in range(LAT)]
            for a, w in enumerate(swap_groups(v)):
                held[TILES * i + t, pl.ds(a, 8, stride=24), :] = w
    for j in range(8 * groups[0], 8 * groups[-1] + 8):
        for t in range(TILES):
            k = 24 * (j % 8)
            level = held[TILES * (j // 8) + t, k : k + 16, :].astype(BF16)
            rows_ref[HALF * j : HALF * (j + 1), 128 * t : 128 * (t + 1)] = level


CHUNK = 512


def updated(rows, table, state):
    return (state.astype(F32) + mm(rows, table).reshape(state.shape)).astype(BF16)


def distance(a, b):
    return jnp.sum(jnp.abs(a.astype(F32) - b.astype(F32)), axis=1)


BLOCKS = [range(0, 3), range(3, GROUPS)]


def own_kernel(where, coef_ref, state_ref, target_ref, table, *rest):
    new_ref, new, skill_ref, held, rows_ref, state, target, sems = rest[-8:]
    levels = pl.ds(pl.multiple_of(HALF * where[0], HALF), HALF)
    loads, stores = [], []
    for k, groups in enumerate(BLOCKS):
        rows = slice(8 * groups[0], 8 * groups[-1] + 8)
        loads.append([
            pltpu.make_async_copy(state_ref.at[rows, levels], state.at[rows], sems.at[0, k]),
            pltpu.make_async_copy(target_ref.at[rows, levels], target.at[rows], sems.at[1, k]),
        ])
        stores.append(
            pltpu.make_async_copy(new.at[rows], new_ref.at[rows, levels], sems.at[2, k])
        )
        for copy in loads[-1]:
            copy.start()
    for k, groups in enumerate(BLOCKS):
        rows = slice(8 * groups[0], 8 * groups[-1] + 8)
        set_rows(coef_ref, held, rows_ref, groups)
        for copy in loads[k]:
            copy.wait()
        for n in range(0, NLON, CHUNK):
            cut = slice(n, n + CHUNK)
            block = rows_ref[HALF * rows.start : HALF * rows.stop]
            value = updated(block, table[:, cut], state[rows, :, cut])
            new[rows, :, cut] = value
            skill_ref[rows, cut] = distance(value, target[rows, :, cut])
        stores[k].start()
    for store in stores:
        store.wait()


def own_step(where, coef, state, target, table, *into):
    return pl.pallas_call(
        own_kernel,
        in_specs=[SMEM, VMEM, HBM, HBM, VMEM] + [HBM for _ in into],
        out_specs=[HBM, VMEM, VMEM],
        out_shape=[
            jax.ShapeDtypeStruct((ROWS, LEVELS, NLON), BF16),
            jax.ShapeDtypeStruct(FIELD, BF16),
            jax.ShapeDtypeStruct((ROWS, NLON), F32),
        ],
        scratch_shapes=[
            pltpu.VMEM((GROUPS * TILES, 8 * 24, 128), F32),
            pltpu.VMEM((ROWS * HALF, NCOL), BF16),
            pltpu.VMEM(FIELD, BF16),
            pltpu.VMEM(FIELD, BF16),
            pltpu.SemaphoreType.DMA((3, 2)),
        ],
        input_output_aliases={5: 0} if into else {},
        cost_estimate=pl.CostEstimate(
            flops=2 * ROWS * HALF * NCOL * NLON, bytes_accessed=14_000_000, transcendentals=0
        ),
        compiler_params=pltpu.CompilerParams(vmem_limit_bytes=OWN_LIMIT),
        name="own_step",
    )(where, coef, state, target, table, *into)


def other_kernel(coef_ref, state_ref, own, table, part_ref, held, rows_ref, state, sems):
    loads = []
    for k, groups in enumerate(BLOCKS):
        rows = slice(8 * groups[0], 8 * groups[-1] + 8)
        loads.append(pltpu.make_async_copy(state_ref.at[rows], state.at[rows], sems.at[k]))
        loads[-1].start()
    for k, groups in enumerate(BLOCKS):
        rows = slice(8 * groups[0], 8 * groups[-1] + 8)
        set_rows(coef_ref, held, rows_ref, groups)
        loads[k].wait()
        for n in range(0, NLON, CHUNK):
            cut = slice(n, n + CHUNK)
            block = rows_ref[HALF * rows.start : HALF * rows.stop]
            value = updated(block, table[:, cut], state[rows, :, cut])
            part_ref[rows, cut] = distance(value, own[rows, :, cut])


def other_step(*operands):
    return pl.pallas_call(
        other_kernel,
        in_specs=[VMEM, HBM, VMEM, VMEM],
        out_specs=VMEM,
        out_shape=jax.ShapeDtypeStruct((ROWS, NLON), F32),
        scratch_shapes=[
            pltpu.VMEM((GROUPS * TILES, 8 * 24, 128), F32),
            pltpu.VMEM((ROWS * HALF, NCOL), BF16),
            pltpu.VMEM(FIELD, BF16),
            pltpu.SemaphoreType.DMA((2,)),
        ],
        cost_estimate=pl.CostEstimate(
            flops=2 * ROWS * HALF * NCOL * NLON, bytes_accessed=12_000_000, transcendentals=0
        ),
        compiler_params=pltpu.CompilerParams(vmem_limit_bytes=SMALL_LIMIT),
        name="other_step",
    )(*operands)


def to_partner(x):
    return lax.ppermute(x, "member", [(0, 1), (1, 0)])


def over_lat(x):
    return lax.all_to_all(x, "lat", split_axis=0, concat_axis=0, tiled=True)


def body(state, target, noise, gain, vertical_mix):
    member = lax.axis_index("member")
    lat = lax.axis_index("lat")
    field = state[0]

    partner_state = to_partner(lax.dynamic_slice_in_dim(field, HALF * (1 - member), HALF, 1))

    table = lon_table()
    sent = forward(field.reshape(ROWS * LEVELS, NLON), jnp.asarray(table))
    gathered = over_lat(sent).reshape(NLAT, OWN * LEVELS)

    mix = jnp.where(member == 1, vertical_mix, jnp.roll(vertical_mix, HALF, axis=0))
    eye = jnp.eye(8, dtype=F32)
    spread = mix.T[:, None, :, None] * eye[None, :, None, :]
    for_noise = jnp.transpose(spread, (1, 0, 2, 3)).reshape(256, 256)
    spread = spread.reshape(256, 256)
    mix_high = spread.astype(BF16)
    mix_low = (spread - lax.reduce_precision(spread, 8, 7)).astype(BF16)
    pick = np.zeros((OWN, OWN * LEVELS), np.float32)
    n = np.arange(OWN * LEVELS)
    pick[8 * (n // 256) + n % 8, n] = math.sqrt(2.0 / NLAT) / math.sqrt(NLON)
    mixed_noise, wide_gain = prepare(
        noise[0].reshape(OWN * LEVELS, NK), for_noise, gain, jnp.asarray(pick)
    )

    high, low = lat_bases()
    bases = [
        np.concatenate([high, low], axis=1),
        np.concatenate([high.transpose(0, 2, 1), low.transpose(0, 2, 1)], axis=1),
    ]
    odd = (lat % 8 >= 4).astype(jnp.int32).reshape(1)
    give, keep = spectral(
        odd, gathered, [jnp.asarray(b) for b in bases], (mix_high, mix_low), mixed_noise, wide_gain
    )
    give = over_lat(give.reshape(LAT, ROWS, TILES * 128))
    partner_coef = to_partner(give)
    keep = over_lat(keep.reshape(LAT, ROWS, TILES * 128))

    back_table = jnp.asarray(np.ascontiguousarray(table.T))
    mine = member.astype(jnp.int32).reshape(1)
    new, _, skill_a = own_step(1 - mine, give, field, target, back_table)
    new, own_half, skill_b = own_step(mine, keep, field, target, back_table, new)
    part = other_step(partner_coef, partner_state, own_half, back_table)
    rest = to_partner(part.astype(BF16)).astype(F32)
    base = (skill_a + skill_b) * F32(1.0 / LEVELS) - part * F32(0.5 / LEVELS)
    crps = lax.optimization_barrier(base) - rest * F32(0.5 / LEVELS)
    return new[None], crps[None]


def solution(mesh):
    placed = (
        P(("ic", "member"), "lat", None, None),
        P(("ic", "lat"), None, None),
        P(("ic", "member"), "lat", None, None),
        P("lat", None),
        P(),
    )

    return jax.shard_map(
        body,
        mesh=mesh,
        in_specs=placed,
        out_specs=(P(("ic", "member"), "lat", None, None), P(("ic", "member"), "lat", None)),
        check_vma=False,
    )
```

```python
import math

import jax
import jax.numpy as jnp
import ml_dtypes
import numpy as np
from jax import lax
from jax.experimental import pallas as pl
from jax.experimental.pallas import tpu as pltpu
from jax.sharding import PartitionSpec as P


NLON = 2560
NLAT = 640
MW = 320
LEVELS = 32
NK = 320
NCOL = 2 * MW
LAT = 16
ROWS = NLAT // LAT
OWN = NCOL // LAT
HALF = LEVELS // 2
TILES = OWN // 8
GROUPS = ROWS // 8
BF16 = jnp.bfloat16
F32 = jnp.float32
HIGHEST = lax.Precision.HIGHEST
OWN_LIMIT = 58 << 20
SMALL_LIMIT = 16 << 20
HBM = pl.BlockSpec(memory_space=pltpu.HBM)
VMEM = pl.BlockSpec(memory_space=pltpu.VMEM)
SMEM = pl.BlockSpec(memory_space=pltpu.SMEM)
FIELD = (ROWS, HALF, NLON)


def column_order():
    n = np.arange(NCOL)
    return 40 * ((n % 128) // 8) + 8 * (n // 128) + n % 8


def lon_table():
    column = column_order()
    part = column // MW
    rest = column % MW
    half = MW // 2
    wave = np.where(rest < half, 2 * rest + 2 * part, 2 * (rest - half) + 1)
    phase = np.arange(NLON)[:, None] * wave[None, :] % NLON
    angle = 2.0 * math.pi / NLON * phase
    table = np.where(part[None, :] == 0, np.cos(angle), np.sin(angle))
    return table.astype(np.float32).astype(ml_dtypes.bfloat16)


def lat_bases():
    theta = (np.arange(NLAT) + 0.5) * (math.pi / NLAT)
    modes = np.arange(NK)
    even = np.cos(modes[:, None] * theta[None, :])
    odd = np.sin((modes[:, None] + 1.0) * theta[None, :])
    both = np.stack([even, odd]).astype(np.float32)
    high = both.astype(ml_dtypes.bfloat16)
    low = (both - high.astype(np.float32)).astype(ml_dtypes.bfloat16)
    return high, low


def turn(x, groups):
    return pltpu.roll(x, 8 * groups % 128, 1) if groups % 16 else x


def swap_groups(v):
    group = lax.broadcasted_iota(jnp.int32, v[0].shape, 1) // 8
    x = [turn(v[-b % 16], -b % 16) for b in range(16)]
    for bit in range(4):
        moved = (group & (1 << bit)) != 0
        x = [jnp.where(moved, x[(g - (1 << bit)) % 16], x[g]) for g in range(16)]
    return [turn(x[g], 16 - g) for g in range(16)]


def forward_kernel(x_ref, table_ref, out_ref, held):
    step = pl.program_id(0)
    now, before = lax.rem(step, 2), lax.rem(step + 1, 2)
    zonal = jnp.dot(x_ref[...], table_ref[...], preferred_element_type=F32)
    for t in range(TILES):
        for h in range(2):
            v = [held[before, t, pl.ds(HALF * h + a, 8, stride=40), :] for a in range(16)]
            lanes = slice(128 * (2 * t + h), 128 * (2 * t + h + 1))
            for q, w in enumerate(swap_groups(v)):
                out_ref[q, :, lanes] = w.astype(BF16)
    for t in range(TILES):
        for j in range(8):
            held[now, t, 40 * j : 40 * j + 32, :] = zonal[
                32 * j : 32 * j + 32, 128 * t : 128 * (t + 1)
            ]


def forward(field, table):
    rows = field.shape[0]
    return pl.pallas_call(
        forward_kernel,
        grid=(GROUPS + 1,),
        in_specs=[
            pl.BlockSpec((rows // GROUPS, NLON), lambda i: (jnp.minimum(i, GROUPS - 1), 0)),
            pl.BlockSpec((NLON, NCOL), lambda i: (0, 0)),
        ],
        out_specs=pl.BlockSpec((LAT, 8, OWN * LEVELS), lambda i: (0, jnp.maximum(i - 1, 0), 0)),
        out_shape=jax.ShapeDtypeStruct((LAT, ROWS, OWN * LEVELS), BF16),
        scratch_shapes=[pltpu.VMEM((2, TILES, 8 * 40, 128), F32)],
        cost_estimate=pl.CostEstimate(
            flops=2 * rows * NLON * NCOL, bytes_accessed=12_000_000, transcendentals=0
        ),
        compiler_params=pltpu.CompilerParams(vmem_limit_bytes=SMALL_LIMIT),
        name="forward_lon",
    )(field, table)


def prepare_kernel(noise_ref, mix_ref, gain_ref, pick_ref, mixed_ref, wide_ref):
    contract = (((0,), (0,)), ((), ()))
    mixed_ref[...] = lax.dot_general(
        noise_ref[...], mix_ref[...], contract, precision=HIGHEST, preferred_element_type=F32
    )
    wide_ref[...] = lax.dot_general(
        gain_ref[...], pick_ref[...], contract, precision=HIGHEST, preferred_element_type=F32
    )


def prepare(noise, mix, gain, pick):
    wide = OWN * LEVELS
    return pl.pallas_call(
        prepare_kernel,
        grid=(TILES,),
        in_specs=[
            pl.BlockSpec((256, NK), lambda t: (t, 0)),
            pl.BlockSpec((256, 256), lambda t: (0, 0)),
            pl.BlockSpec((OWN, NK), lambda t: (0, 0)),
            pl.BlockSpec((OWN, 256), lambda t: (0, t)),
        ],
        out_specs=[
            pl.BlockSpec((NK, 256), lambda t: (0, t)),
            pl.BlockSpec((NK, 256), lambda t: (0, t)),
        ],
        out_shape=[jax.ShapeDtypeStruct((NK, wide), F32)] * 2,
        cost_estimate=pl.CostEstimate(
            flops=12 * 256 * NK * wide, bytes_accessed=6_000_000, transcendentals=0
        ),
        compiler_params=pltpu.CompilerParams(vmem_limit_bytes=SMALL_LIMIT),
        name="prepare_noise",
    )(noise, mix, gain, pick)


def halves(x):
    high = x.astype(BF16)
    return high, (x - high.astype(F32)).astype(BF16)


def mm(a, b):
    return jnp.dot(a, b, preferred_element_type=F32)


def spectral_kernel(odd, g_ref, b_ref, t_ref, mh_ref, ml_ref, noise_ref, gain_ref, send_ref, keep_ref, b, t, noise, gain, sems):
    loads = [
        pltpu.make_async_copy(b_ref.at[odd[0]], b, sems.at[0]),
        pltpu.make_async_copy(gain_ref, gain, sems.at[1]),
        pltpu.make_async_copy(noise_ref, noise, sems.at[2]),
        pltpu.make_async_copy(t_ref.at[odd[0]], t, sems.at[3]),
    ]
    for copy in loads:
        copy.start()
    loads[0].wait()
    for k in range(TILES):
        lanes = slice(256 * k, 256 * (k + 1))
        both = mm(b[...], g_ref[:, lanes])
        if k == 0:
            loads[1].wait()
        forced = (both[:NK] + both[NK:]) * gain[:, lanes]
        high, low = halves(forced)
        both = mm(jnp.concatenate([high, low], axis=0), mh_ref[...])
        if k == 0:
            loads[2].wait()
        mixed = both[:NK] + both[NK:] + mm(high, ml_ref[...]) + noise[:, lanes]
        high, low = halves(mixed)
        if k == 0:
            loads[3].wait()
        both = mm(t[...], high)
        back = both[:NLAT] + both[NLAT:] + mm(t[:NLAT], low)
        back = (back * F32(math.sqrt(2.0) / NK)).astype(BF16)
        send_ref[:, 128 * k : 128 * (k + 1)] = back[:, :128]
        keep_ref[:, 128 * k : 128 * (k + 1)] = back[:, 128:]


def spectral(odd, gathered, bases, mixes, noise, gain):
    return pl.pallas_call(
        spectral_kernel,
        in_specs=[SMEM, VMEM, HBM, HBM, VMEM, VMEM, HBM, HBM],
        out_specs=[VMEM, VMEM],
        out_shape=[jax.ShapeDtypeStruct((NLAT, TILES * 128), BF16)] * 2,
        scratch_shapes=[
            pltpu.VMEM((2 * NK, NLAT), BF16),
            pltpu.VMEM((2 * NLAT, NK), BF16),
            pltpu.VMEM((NK, OWN * LEVELS), F32),
            pltpu.VMEM((NK, OWN * LEVELS), F32),
            pltpu.SemaphoreType.DMA((4,)),
        ],
        cost_estimate=pl.CostEstimate(
            flops=4_000_000_000, bytes_accessed=10_000_000, transcendentals=0
        ),
        compiler_params=pltpu.CompilerParams(vmem_limit_bytes=OWN_LIMIT),
        name="spectral_step",
    )(odd, gathered, *bases, *mixes, noise, gain)


def set_rows(coef_ref, held, rows_ref, groups):
    for i in groups:
        for t in range(TILES):
            lanes = slice(128 * t, 128 * (t + 1))
            v = [coef_ref[q, 8 * i : 8 * i + 8, lanes].astype(F32) for q in range(LAT)]
            for a, w in enumerate(swap_groups(v)):
                held[TILES * i + t, pl.ds(a, 8, stride=24), :] = w
    for j in range(8 * groups[0], 8 * groups[-1] + 8):
        for t in range(TILES):
            k = 24 * (j % 8)
            level = held[TILES * (j // 8) + t, k : k + 16, :].astype(BF16)
            rows_ref[HALF * j : HALF * (j + 1), 128 * t : 128 * (t + 1)] = level


CHUNK = 512


def updated(rows, table, state):
    return (state.astype(F32) + mm(rows, table).reshape(state.shape)).astype(BF16)


def distance(a, b):
    return jnp.sum(jnp.abs(a.astype(F32) - b.astype(F32)), axis=1)


BLOCKS = [range(0, 3), range(3, GROUPS)]


def own_kernel(where, coef_ref, state_ref, target_ref, table_ref, *rest):
    new_ref, skill_ref, new, held, rows_ref, state, target, table, sems = rest[-9:]
    levels = pl.ds(pl.multiple_of(HALF * where[0], HALF), HALF)
    whole = pltpu.make_async_copy(table_ref, table, sems.at[3, 0])
    loads, stores = [], []
    for k, groups in enumerate(BLOCKS):
        rows = slice(8 * groups[0], 8 * groups[-1] + 8)
        loads.append([
            pltpu.make_async_copy(state_ref.at[rows, levels], state.at[rows], sems.at[0, k]),
            pltpu.make_async_copy(target_ref.at[rows, levels], target.at[rows], sems.at[1, k]),
        ])
        stores.append(
            pltpu.make_async_copy(new.at[rows], new_ref.at[rows, levels], sems.at[2, k])
        )
        for copy in loads[-1]:
            copy.start()
        if k == 0:
            whole.start()
    for k, groups in enumerate(BLOCKS):
        rows = slice(8 * groups[0], 8 * groups[-1] + 8)
        set_rows(coef_ref, held, rows_ref, groups)
        for copy in loads[k]:
            copy.wait()
        if k == 0:
            whole.wait()
        for n in range(0, NLON, CHUNK):
            cut = slice(n, n + CHUNK)
            block = rows_ref[HALF * rows.start : HALF * rows.stop]
            value = updated(block, table[:, cut], state[rows, :, cut])
            new[rows, :, cut] = value
            skill_ref[rows, cut] = distance(value, target[rows, :, cut])
        stores[k].start()
    for store in stores:
        store.wait()


def own_step(where, coef, state, target, table, *into):
    return pl.pallas_call(
        own_kernel,
        in_specs=[SMEM, VMEM, HBM, HBM, HBM] + [HBM for _ in into],
        out_specs=[HBM, VMEM, VMEM] if into else [HBM, VMEM],
        out_shape=[
            jax.ShapeDtypeStruct((ROWS, LEVELS, NLON), BF16),
            jax.ShapeDtypeStruct((ROWS, NLON), F32),
        ]
        + [jax.ShapeDtypeStruct(FIELD, BF16) for _ in into],
        scratch_shapes=([] if into else [pltpu.VMEM(FIELD, BF16)])
        + [
            pltpu.VMEM((GROUPS * TILES, 8 * 24, 128), F32),
            pltpu.VMEM((ROWS * HALF, NCOL), BF16),
            pltpu.VMEM(FIELD, BF16),
            pltpu.VMEM(FIELD, BF16),
            pltpu.VMEM((NCOL, NLON), BF16),
            pltpu.SemaphoreType.DMA((4, 2)),
        ],
        input_output_aliases={5: 0} if into else {},
        cost_estimate=pl.CostEstimate(
            flops=2 * ROWS * HALF * NCOL * NLON, bytes_accessed=14_000_000, transcendentals=0
        ),
        compiler_params=pltpu.CompilerParams(vmem_limit_bytes=OWN_LIMIT),
        name="own_step",
    )(where, coef, state, target, table, *into)


def other_kernel(coef_ref, state_ref, own, table, part_ref, held, rows_ref, state, sems):
    loads = []
    for k, groups in enumerate(BLOCKS):
        rows = slice(8 * groups[0], 8 * groups[-1] + 8)
        loads.append(pltpu.make_async_copy(state_ref.at[rows], state.at[rows], sems.at[k]))
        loads[-1].start()
    for k, groups in enumerate(BLOCKS):
        rows = slice(8 * groups[0], 8 * groups[-1] + 8)
        set_rows(coef_ref, held, rows_ref, groups)
        loads[k].wait()
        for n in range(0, NLON, CHUNK):
            cut = slice(n, n + CHUNK)
            block = rows_ref[HALF * rows.start : HALF * rows.stop]
            value = updated(block, table[:, cut], state[rows, :, cut])
            part_ref[rows, cut] = distance(value, own[rows, :, cut])


def other_step(*operands):
    return pl.pallas_call(
        other_kernel,
        in_specs=[VMEM, HBM, VMEM, VMEM],
        out_specs=VMEM,
        out_shape=jax.ShapeDtypeStruct((ROWS, NLON), F32),
        scratch_shapes=[
            pltpu.VMEM((GROUPS * TILES, 8 * 24, 128), F32),
            pltpu.VMEM((ROWS * HALF, NCOL), BF16),
            pltpu.VMEM(FIELD, BF16),
            pltpu.SemaphoreType.DMA((2,)),
        ],
        cost_estimate=pl.CostEstimate(
            flops=2 * ROWS * HALF * NCOL * NLON, bytes_accessed=12_000_000, transcendentals=0
        ),
        compiler_params=pltpu.CompilerParams(vmem_limit_bytes=SMALL_LIMIT),
        name="other_step",
    )(*operands)


def to_partner(x):
    return lax.ppermute(x, "member", [(0, 1), (1, 0)])


def over_lat(x):
    return lax.all_to_all(x, "lat", split_axis=0, concat_axis=0, tiled=True)


def body(state, target, noise, gain, vertical_mix):
    member = lax.axis_index("member")
    lat = lax.axis_index("lat")
    field = state[0]

    partner_state = to_partner(lax.dynamic_slice_in_dim(field, HALF * (1 - member), HALF, 1))

    table = lon_table()
    sent = forward(field.reshape(ROWS * LEVELS, NLON), jnp.asarray(table))
    gathered = over_lat(sent).reshape(NLAT, OWN * LEVELS)

    mix = jnp.where(member == 1, vertical_mix, jnp.roll(vertical_mix, HALF, axis=0))
    eye = jnp.eye(8, dtype=F32)
    spread = mix.T[:, None, :, None] * eye[None, :, None, :]
    for_noise = jnp.transpose(spread, (1, 0, 2, 3)).reshape(256, 256)
    spread = spread.reshape(256, 256)
    mix_high = spread.astype(BF16)
    mix_low = (spread - lax.reduce_precision(spread, 8, 7)).astype(BF16)
    pick = np.zeros((OWN, OWN * LEVELS), np.float32)
    n = np.arange(OWN * LEVELS)
    pick[8 * (n // 256) + n % 8, n] = math.sqrt(2.0 / NLAT) / math.sqrt(NLON)
    mixed_noise, wide_gain = prepare(
        noise[0].reshape(OWN * LEVELS, NK), for_noise, gain, jnp.asarray(pick)
    )

    high, low = lat_bases()
    bases = [
        np.concatenate([high, low], axis=1),
        np.concatenate([high.transpose(0, 2, 1), low.transpose(0, 2, 1)], axis=1),
    ]
    odd = (lat % 8 >= 4).astype(jnp.int32).reshape(1)
    give, keep = spectral(
        odd, gathered, [jnp.asarray(b) for b in bases], (mix_high, mix_low), mixed_noise, wide_gain
    )
    give = over_lat(give.reshape(LAT, ROWS, TILES * 128))
    partner_coef = to_partner(give)
    keep = over_lat(keep.reshape(LAT, ROWS, TILES * 128))

    back_table = jnp.asarray(np.ascontiguousarray(table.T))
    mine = member.astype(jnp.int32).reshape(1)
    new, skill_a = own_step(1 - mine, give, field, target, back_table)
    new, skill_b, own_half = own_step(mine, keep, field, target, back_table, new)
    part = other_step(partner_coef, partner_state, own_half, back_table)
    rest = to_partner(part.astype(BF16)).astype(F32)
    base = (skill_a + skill_b) * F32(1.0 / LEVELS) - part * F32(0.5 / LEVELS)
    crps = lax.optimization_barrier(base) - rest * F32(0.5 / LEVELS)
    return new[None], crps[None]


def solution(mesh):
    placed = (
        P(("ic", "member"), "lat", None, None),
        P(("ic", "lat"), None, None),
        P(("ic", "member"), "lat", None, None),
        P("lat", None),
        P(),
    )

    return jax.shard_map(
        body,
        mesh=mesh,
        in_specs=placed,
        out_specs=(P(("ic", "member"), "lat", None, None), P(("ic", "member"), "lat", None)),
        check_vma=False,
    )
```
